256 devices in a mesh: grp: 4 (over z_hi), ep: 32 (over y, x, z_lo), tp: 2 (over core).
Axes of the slice: x: 4, y: 4, z: 8 (z_hi: 4, z_lo: 2; z = z_hi * 2 + z_lo), core: 2. Of those that a mesh axis runs over, the one named last changes fastest.
Arguments:
- tokens: bfloat16 [1024, 7168], P('ep', 'tp'), may hold values from -6 to 6
- gates: float32 [1024, 8], P('ep'), may hold values from 0.05 to 1
- expert_ids: int32 [1024, 8], P('ep'), may hold values from 0 to 31, all different within a row; in each aligned block of 16 rows (0 to 15, 16 to 31, ...) at most 8 rows name the same one
- gate_weight: bfloat16 [32, 7168, 2048], P('ep', None, ('grp', 'tp')), may hold values from -0.0625 to 0.0625
- up_weight: bfloat16 [32, 7168, 2048], P('ep', None, ('grp', 'tp')), may hold values from -0.0625 to 0.0625
- down_weight: bfloat16 [32, 2048, 7168], P('ep', ('grp', 'tp')), may hold values from -0.125 to 0.125
Outputs:
- mixed_out: bfloat16 [1024, 7168], P('ep', ('grp', 'tp'))
The draws below stay inside these ranges and needn't reach their ends.
Inputs may be any that keep to these rules, and one draw needn't show every extreme that they name: `expert_ids`: within each aligned block of 16 rows, the 8 experts of a row differ, and no expert is named by more than 8 rows; some expert is named by exactly 8 rows in some blocks.
All inputs are finite; a program needn't handle non-finite values.
Results may differ from the reference program's by a relative error of at most 0.013.
Values may be sent and summed in bfloat16 or wider, within the bound.
No kernel may reach another device: no remote copies, remote signals or barrier semaphores. Data moves between devices by JAX's collectives and lax.ppermute only.
A program may use at most 128 MiB of HBM per device.

```python
import math
import jax
import jax.numpy as jnp
import numpy as np
from jax import lax

D = 7168
FF = 2048
TOP = 8
EXPERTS = 32
TOK_MB = 16
CAP = 8
TOKENS = 1024


def levels(own_key, shape, cuts, smallest, largest):
    gain = 1.0
    for dim, shards_of in cuts:
        steps = jax.random.uniform(jax.random.fold_in(jax.random.fold_in(own_key, 6), dim), (shards_of,), jnp.float32, smallest / len(cuts), largest / len(cuts))
        gain = gain * jnp.repeat(jnp.exp(steps), shape[dim] // shards_of).reshape((-1,) + (1,) * (len(shape) - 1 - dim))
    return gain


def routed_block(stream_key, own, number, rows, number_of, top, most, skew):
    ranking = jax.random.permutation(stream_key, number_of)
    packed, common = shares(number_of, rows * top, most, skew, True), shares(number_of, rows * top, most, skew, False)
    places = jnp.arange(number_of)

    def named(lengths, turn):
        used = int((lengths > 0).sum())
        fixed = max(1, used // 4)
        shifted = fixed + (places - fixed + turn * (used - fixed)) % max(1, number_of - fixed)
        return jnp.zeros((number_of,), jnp.int32).at[ranking[jnp.where(places < fixed, places, shifted)]].set(jnp.asarray(lengths, jnp.int32))

    lengths = jnp.where(number % 4 == 0, named(packed, number // 4), named(common, number - number // 4 - 1))
    mixed = jax.random.permutation(jax.random.fold_in(own, 3), number_of)
    donor, sink = mixed[0:number_of // 2 * 2:2], mixed[1:number_of // 2 * 2:2]
    room = jnp.minimum(lengths[donor] - 1, most - lengths[sink]) // 2
    room = jnp.where((donor == ranking[0]) | (sink == ranking[0]) | (lengths[sink] == 0), 0, jnp.maximum(room, 0))
    shifted = jax.random.randint(jax.random.fold_in(own, 4), (number_of // 2,), 0, 1 << 20) % (room + 1)
    lengths = lengths.at[donor].add(-shifted).at[sink].add(shifted)
    items = jnp.searchsorted(jnp.cumsum(lengths), jnp.arange(rows * top), side="right").astype(jnp.int32)
    grid = items.reshape(top, rows).T
    grid = grid[jax.random.permutation(jax.random.fold_in(own, 1), rows)]
    turn = jax.random.randint(jax.random.fold_in(own, 2), (rows, 1), 0, top)
    return jnp.take_along_axis(grid, (jnp.arange(top)[None, :] + turn) % top, axis=1)


def shares(amount, total, limit, skew, full):
    portions = [(1 << 20) // math.isqrt(grade ** skew) + 1 for grade in range(1, amount + 1)]
    largest = limit if full else min(limit, max(-(-total // amount), total * portions[0] // sum(portions)))
    least = 1 if total - largest >= amount - 1 else 0
    counts, surplus = [largest] + [least] * (amount - 1), total - largest - least * (amount - 1)
    while surplus > 0:
        candidates = [i for i in range(1, amount) if counts[i] < largest] or [i for i in range(1, amount) if counts[i] < limit]
        mass, remaining = sum([portions[i] for i in candidates]), surplus
        for i in candidates:
            extra = min(limit - counts[i], max(1, remaining * portions[i] // mass), surplus)
            counts[i] = counts[i] + extra
            surplus = surplus - extra
    return np.array(counts)


def scatter_about(rng, shape, deviation, most, pieces=(), kind=jnp.bfloat16):
    entries = deviation * jax.random.normal(rng, shape, jnp.float32)
    if pieces:
        entries = entries * levels(rng, shape, pieces, -0.22, 0.18)
    return jnp.clip(entries, -most, most).astype(kind)


def setup_inputs(seed: int = 0) -> dict:
    key_of = jax.random.split(jax.random.key(seed), 7)
    tokens = scatter_about(key_of[0], (TOKENS, D), 1.0, 6.0, ((0, 32), (1, 2)))
    gates = jnp.clip(jnp.exp(math.log(1.0) - 2.9957323 * jax.random.uniform(key_of[1], (TOKENS, TOP), jnp.float32) ** levels(key_of[1], (TOKENS, TOP), ((0, 32),), -0.2, 0.2)), 0.05, 1.0)
    expert_ids_keys = jax.random.split(jax.random.fold_in(key_of[2], 1), TOKENS // TOK_MB)
    expert_ids_turns = jax.random.permutation(jax.random.fold_in(key_of[2], 3), TOKENS // TOK_MB)
    expert_ids = jax.vmap(lambda own, number: routed_block(jax.random.fold_in(key_of[2], 2), own, number, TOK_MB, EXPERTS, TOP, CAP, 2))(expert_ids_keys, expert_ids_turns).reshape((TOKENS, TOP))
    gate_weight = scatter_about(key_of[3], (EXPERTS, D, FF), D ** -0.5, 0.0625, ((0, 32), (2, 8)))
    up_weight = scatter_about(key_of[4], (EXPERTS, D, FF), D ** -0.5, 0.0625, ((0, 32), (2, 8)))
    down_weight = scatter_about(key_of[5], (EXPERTS, FF, D), FF ** -0.5, 0.125, ((0, 32), (1, 8)))
    return dict(tokens=tokens, gates=gates, expert_ids=expert_ids, gate_weight=gate_weight, up_weight=up_weight, down_weight=down_weight)


def reference(tokens, gates, expert_ids, gate_weight, up_weight, down_weight):
    blocks = TOKENS // TOK_MB
    assigned = expert_ids.reshape(blocks, TOK_MB * TOP).astype(jnp.int32)
    labels = jnp.arange(EXPERTS, dtype=jnp.int32)
    onehot = (assigned[:, :, None] == labels[None, None, :]).astype(jnp.int32)
    before = jnp.cumsum(onehot, axis=1) - onehot
    slot = jnp.sum(before * onehot, axis=2).astype(jnp.int32)
    position = jnp.arange(TOK_MB * TOP, dtype=jnp.int32)
    block_rows = jnp.arange(blocks, dtype=jnp.int32)
    owner_row = (block_rows[:, None] * TOK_MB + position[None, :] // TOP).astype(jnp.int32)
    block_index = jnp.broadcast_to(block_rows[:, None], assigned.shape)
    table = jnp.full((blocks, EXPERTS, CAP), TOKENS, jnp.int32).at[block_index, assigned, slot].set(owner_row)
    weight_table = jnp.zeros((blocks, EXPERTS, CAP), jnp.float32).at[block_index, assigned, slot].set(
        gates.reshape(blocks, TOK_MB * TOP).astype(jnp.float32))
    padded = jnp.concatenate([tokens, jnp.zeros((1, D), tokens.dtype)], axis=0)

    def apply(total, expert):
        picked = table[:, expert].reshape(-1)
        scale = weight_table[:, expert].reshape(-1)
        rows = padded[picked].astype(jnp.float32)
        gate = jnp.dot(rows, gate_weight[expert].astype(jnp.float32), preferred_element_type=jnp.float32)
        upper = jnp.dot(rows, up_weight[expert].astype(jnp.float32), preferred_element_type=jnp.float32)
        hidden = lax.optimization_barrier((jax.nn.silu(gate) * upper).astype(jnp.bfloat16)).astype(jnp.float32)
        result = jnp.dot(hidden, down_weight[expert].astype(jnp.float32), preferred_element_type=jnp.float32)
        result = lax.optimization_barrier(result.astype(jnp.bfloat16)).astype(jnp.float32)
        return total.at[picked].add(scale[:, None] * result), None

    start = jnp.zeros((TOKENS + 1, D), jnp.float32)
    total, unused = lax.scan(apply, start, jnp.arange(EXPERTS, dtype=jnp.int32))
    return total[:TOKENS].astype(jnp.bfloat16)
```

```python
import jax
import jax.numpy as jnp
from jax import lax
from jax.experimental import pallas as pl
from jax.experimental.pallas import tpu as pltpu
from jax.sharding import Mesh
from jax.sharding import PartitionSpec as P

CAP = 8
TOK_MB = 16
INTERPRET = False
Z = ("grp", "zl")
BF = jnp.bfloat16
F32 = jnp.float32


def shift(a, axis, d):
    n = lax.axis_size(axis)
    return lax.ppermute(a, axis, [((i + d) % n, i) for i in range(n)])


def ring_gather(own, other, axis):
    left0, right0 = shift(own, axis, -1), shift(own, axis, 1)
    left1, right1 = shift(other, axis, -1), shift(other, axis, 1)
    far0 = shift(left0, axis, -1)
    far1 = shift(right1, axis, 1)
    return [own, other, right0, right1, far0, far1, left0, left1]


def slots_exchange(pieces, axis):
    here, right, far_a, far_b, left = pieces
    mid_a, mid_b = shift(far_a, axis, -1), shift(far_b, axis, 1)
    from_left, from_right = shift(right, axis, -1), shift(left, axis, 1)
    from_far_a, from_far_b = shift(mid_a, axis, -1), shift(mid_b, axis, 1)
    return [here, from_right, from_far_a, from_far_b, from_left]


def add(*terms):
    total = terms[0].astype(F32)
    for term in terms[1:]:
        total = total + term.astype(F32)
    return total.astype(BF)


def ring_scatter(d, axis):
    part_a, part_b = shift(d[4], axis, -1), shift(d[5], axis, 1)
    plain_a, plain_b = shift(d[3], axis, -1), shift(d[6], axis, 1)
    full_a = shift(add(d[2], part_a), axis, -1)
    full_b = shift(add(d[7], part_b), axis, 1)
    return add(d[0], full_a, plain_b), add(d[1], plain_a, full_b)


def piece_rows(slots):
    q = slots // 4
    return [(0, q), (q, q), (2 * q, q // 2), (2 * q + q // 2, q // 2), (3 * q, q)]


def vmem():
    return pl.BlockSpec(memory_space=pltpu.VMEM)


def select_kernel(*refs):
    tokens, onehot, outs = refs[:8], refs[8], refs[9:]
    rows = jnp.concatenate([r[...] for r in tokens], axis=0)
    picked = jnp.dot(onehot[...], rows, preferred_element_type=F32).astype(BF)
    for out, (start, size) in zip(outs, piece_rows(onehot.shape[0])):
        out[...] = picked[start : start + size]


def select(tokens, onehot):
    width = tokens[0].shape[1]
    return pl.pallas_call(
        select_kernel,
        out_shape=[jax.ShapeDtypeStruct((n, width), BF) for _, n in piece_rows(onehot.shape[0])],
        in_specs=[vmem()] * 9,
        out_specs=[vmem()] * 5,
        interpret=INTERPRET,
        name="select",
    )(*tokens, onehot)


def spread_kernel(*refs):
    pieces, onehot, outs = refs[:5], refs[5], refs[6:]
    rows = jnp.concatenate([r[...] for r in pieces], axis=0)
    total = lax.dot_general(
        onehot[...], rows, (((0,), (0,)), ((), ())), preferred_element_type=F32
    ).astype(BF)
    size = total.shape[0] // 8
    for i, out in enumerate(outs):
        out[...] = total[i * size : (i + 1) * size]


def spread(pieces, onehot):
    width = pieces[0].shape[1]
    return pl.pallas_call(
        spread_kernel,
        out_shape=[jax.ShapeDtypeStruct((onehot.shape[1] // 8, width), BF)] * 8,
        in_specs=[vmem()] * 6,
        out_specs=[vmem()] * 8,
        interpret=INTERPRET,
        name="spread",
    )(*pieces, onehot)


def swapped(x):
    size = x.shape[0] // 16
    return jnp.concatenate(
        [x[(a * 4 + b) * size : (a * 4 + b + 1) * size] for b in range(4) for a in range(4)], axis=0
    )


def hidden_body(t, *refs):
    groups = [refs[5 * i : 5 * i + 5] for i in range(4)]
    scale, gate, up, out_a, out_b, acc = refs[20:]
    step = pl.program_id(0)
    width = gate.shape[1]
    for i in range(4):

        @pl.when(step == i)
        def _(i=i):
            x = jnp.concatenate([r[...] for r in groups[i]], axis=0)
            g = jnp.dot(x, gate[...], preferred_element_type=F32)
            u = jnp.dot(x, up[...], preferred_element_type=F32)
            if i < 2:
                acc[i, :, :width] = g
                acc[i, :, width:] = u
            else:
                acc[i - 2, :, :width] += g
                acc[i - 2, :, width:] += u

    @pl.when(step == 3)
    def _():
        total = acc[0] + swapped(acc[1])
        g, u = total[:, :width], total[:, width:]
        hidden = (g * jax.nn.sigmoid(g) * u * scale[...]).astype(BF)
        out_a[...] = hidden
        out_b[...] = swapped(hidden)


def hidden_of(own_a, own_b, peer_a, peer_b, scale, gate, up, t):
    depth, width = gate.shape
    slots = scale.shape[0]
    block = depth // 4

    def rows(i, t_ref):
        mine = t_ref[0]
        return jnp.where(i < 2, 2 * mine + i, 2 * (1 - mine) + i - 2), 0

    weight = pl.BlockSpec((block, width), rows)
    return pl.pallas_call(
        hidden_body,
        out_shape=[jax.ShapeDtypeStruct((slots, width), BF)] * 2,
        grid_spec=pltpu.PrefetchScalarGridSpec(
            num_scalar_prefetch=1,
            grid=(4,),
            in_specs=[vmem()] * 21 + [weight, weight],
            out_specs=[vmem()] * 2,
            scratch_shapes=[pltpu.VMEM((2, slots, 2 * width), F32)],
        ),
        interpret=INTERPRET,
        name="hidden",
    )(t, *own_a, *own_b, *peer_a, *peer_b, scale, gate, up)


def down_body(t, hidden, weight, out):
    out[...] = jnp.dot(hidden[...], weight[...], preferred_element_type=F32).astype(BF)


def down_add_body(t, hidden, weight, term, *outs):
    total = jnp.dot(hidden[...], weight[...], preferred_element_type=F32) + term[...].astype(F32)
    total = total.astype(BF)
    for out, (start, size) in zip(outs, piece_rows(hidden.shape[0])):
        out[...] = total[start : start + size]


def down(hidden, weight, which, first, term=None):
    slots, inner = hidden.shape
    block = weight.shape[1] // 8
    columns = pl.BlockSpec((inner, block), lambda i, t: (0, 2 * (first + i) + t[0]))
    ins = [pl.BlockSpec((slots, inner), lambda i, t: (0, 0)), columns]
    if term is None:
        sizes, body, args = [slots], down_body, ()
    else:
        sizes, body, args = [n for _, n in piece_rows(slots)], down_add_body, (term,)
        ins.append(pl.BlockSpec((slots, block), lambda i, t: (0, i)))
    outs = pl.pallas_call(
        body,
        out_shape=[jax.ShapeDtypeStruct((n, 2 * block), BF) for n in sizes],
        grid_spec=pltpu.PrefetchScalarGridSpec(
            num_scalar_prefetch=1,
            grid=(2,),
            in_specs=ins,
            out_specs=[pl.BlockSpec((n, block), lambda i, t: (0, i)) for n in sizes],
        ),
        interpret=INTERPRET,
        name="down" if term is None else "down_add",
    )(which, hidden, weight, *args)
    return outs[0] if term is None else outs


def places(ids, experts):
    chosen = jnp.sum((ids.T[None] == experts[:, None, None]).astype(F32), axis=1)
    blocks = chosen.reshape(-1, TOK_MB)
    i = lax.broadcasted_iota(jnp.int32, (TOK_MB, TOK_MB), 0)
    j = lax.broadcasted_iota(jnp.int32, (TOK_MB, TOK_MB), 1)
    before = jnp.dot(blocks, (i < j).astype(F32), preferred_element_type=F32)
    return chosen, before.reshape(chosen.shape)


def onehots(ids, experts):
    chosen, before = places(ids, experts)
    tokens = ids.shape[0]
    slots = tokens // TOK_MB * CAP
    r = lax.broadcasted_iota(jnp.int32, (slots, tokens), 0)
    c = lax.broadcasted_iota(jnp.int32, (slots, tokens), 1)
    target = jnp.where(chosen > 0.5, before, -1.0)[:, None, :]
    hit = (r // CAP == c // TOK_MB)[None] & (target == (r % CAP).astype(F32)[None])
    return hit.astype(BF).reshape(-1, tokens)


def local(tokens, gates, expert_ids, gate_weight, up_weight, down_weight):
    gate, up, downw = gate_weight[0], up_weight[0], down_weight[0]
    y, x, zl, t = (lax.axis_index(a) for a in ("y", "x", "zl", "tp"))
    half = tokens.shape[1] // 2
    own_a, own_b = tokens[:, :half], tokens[:, half:]

    meta = jnp.concatenate([expert_ids.astype(F32), gates], axis=1)
    meta = jnp.concatenate([meta, shift(meta, "zl", 1)], axis=0)
    for axis in ("y", "x"):
        meta = jnp.concatenate([meta] + [shift(meta, axis, d) for d in (1, 2, 3)], axis=0)
    per_place = meta.shape[0] // 16
    grid = meta.reshape(4, 4, per_place, 16)
    ids_a = meta[: 4 * per_place, :8]
    ids_b = grid[:, 0].reshape(4 * per_place, 16)[:, :8]
    offsets = jnp.arange(4, dtype=jnp.int32)
    experts_a = (y * 8 + (x + offsets) % 4 * 2 + zl).astype(F32)
    experts_b = ((y + offsets) % 4 * 8 + x * 2 + zl).astype(F32)
    oh_a, oh_b = onehots(ids_a, experts_a), onehots(ids_b, experts_b)
    chosen, before = places(meta[:, :8], experts_a[:1])
    mine = jnp.sum(jnp.where(meta[:, :8] == experts_a[0], meta[:, 8:], 0.0), axis=1)
    target = jnp.where(chosen > 0.5, before, -1.0).reshape(-1, 1, TOK_MB)
    slot = lax.broadcasted_iota(jnp.int32, (1, CAP, 1), 1).astype(F32)
    scale = jnp.sum(jnp.where(target == slot, mine.reshape(-1, 1, TOK_MB), 0.0), axis=2)
    scale = scale.reshape(-1, 1)

    other_a, other_b = shift(own_a, Z, 1), shift(own_b, Z, -1)
    rows_a, rows_b = ring_gather(own_a, other_a, "y"), ring_gather(own_b, other_b, "x")
    got_a = slots_exchange(select(rows_a, oh_a), "x")
    got_b = slots_exchange(select(rows_b, oh_b), "y")
    peer_a, peer_b = [shift(p, "tp", 1) for p in got_a], [shift(p, "tp", 1) for p in got_b]
    which = t.astype(jnp.int32).reshape(1)
    hid_a, hid_b = hidden_of(got_a, got_b, peer_a, peer_b, scale, gate, up, which)
    sent_a = shift(down(hid_a, downw, 1 - which, 0), "tp", 1)
    sent_b = shift(down(hid_b, downw, 1 - which, 2), "tp", 1)
    back_a = slots_exchange(down(hid_a, downw, which, 0, sent_a), "x")
    back_b = slots_exchange(down(hid_b, downw, which, 2, sent_b), "y")
    near_a, away_a = ring_scatter(spread(back_a, oh_a), "y")
    near_b, away_b = ring_scatter(spread(back_b, oh_b), "x")
    total_a = add(near_a, shift(away_a, Z, -1))
    total_b = add(near_b, shift(away_b, Z, 1))
    rows, wide = total_a.shape
    blocks = [total_a[:, : wide // 2], total_a[:, wide // 2 :], total_b[:, : wide // 2], total_b[:, wide // 2 :]]
    shares = lax.all_to_all(jnp.stack(blocks), "grp", split_axis=0, concat_axis=0, tiled=True)
    return jnp.sum(shares.astype(F32), axis=0).astype(BF)


def solution(mesh):
    fine = Mesh(mesh.devices.reshape(4, 4, 4, 2, 2), ("grp", "y", "x", "zl", "tp"))
    ep = ("y", "x", "zl")
    placed = (
        P(ep, "tp"),
        P(ep, None),
        P(ep, None),
        P(ep, None, ("grp", "tp")),
        P(ep, None, ("grp", "tp")),
        P(ep, ("grp", "tp"), None),
    )
    return jax.shard_map(
        local, mesh=fine, in_specs=placed, out_specs=P(ep, ("grp", "tp")), check_vma=False
    )
```

```python
import jax
import jax.numpy as jnp
from jax import lax
from jax.experimental import pallas as pl
from jax.experimental.pallas import tpu as pltpu
from jax.sharding import Mesh
from jax.sharding import PartitionSpec as P

TOP = 8
CAP = 8
TOK_MB = 16
META = 128
GATES_AT = 32
INTERPRET = False
Z = ("grp", "zl")
BF = jnp.bfloat16
F32 = jnp.float32


def params(mib):
    return pltpu.CompilerParams(vmem_limit_bytes=mib << 20)


def vmem():
    return pl.BlockSpec(memory_space=pltpu.VMEM)


def shift(a, axis, d):
    n = lax.axis_size(axis)
    return lax.ppermute(a, axis, [((i + d) % n, i) for i in range(n)])


def add(*terms):
    total = terms[0].astype(F32)
    for term in terms[1:]:
        total = total + term.astype(F32)
    return total.astype(BF)


def ring_gather(own, other, axis):
    both = jnp.concatenate([own, other], axis=0)
    right = shift(both, axis, 1)
    left = shift(both, axis, -1)
    far_a = shift(own, axis, 2)
    far_b = shift(right[own.shape[0] :], axis, 1)
    return [both, right, far_a, far_b, left]


def slots_exchange(pieces, axis):
    here, right, far, left_far = pieces
    got = shift(left_far, axis, 1)
    from_left = shift(right, axis, -1)
    far_a = shift(far, axis, 2)
    far_b = shift(got[right.shape[0] :], axis, 1)
    return [here, got, far_a, far_b, from_left]


def ring_scatter(here, right, far_a, far_b, left_a, left_b, axis):
    relay = shift(far_b, axis, 1)
    from_left = shift(right, axis, -1)
    direct = shift(far_a, axis, 2)
    from_right = shift(jnp.concatenate([left_a, add(left_b, relay)], axis=0), axis, 1)
    n = far_a.shape[0]
    own = add(here[:n], from_left[:n], from_right[:n], direct)
    other = add(here[n:], from_left[n:], from_right[n:])
    return own, other


def out_pieces(x, outs):
    q = x.shape[0] // 4
    outs[0][...] = x[:q]
    outs[1][...] = x[q : 2 * q]
    outs[2][...] = x[2 * q : 2 * q + q // 2]
    outs[3][:q] = x[3 * q :]
    outs[3][q:] = x[2 * q + q // 2 : 3 * q]


def piece_rows(slots):
    q = slots // 4
    return [q, q, q // 2, q + q // 2]


def in_rows(refs, columns):
    q = refs[0].shape[0]
    return jnp.concatenate(
        [r[:q, columns] if i == 1 else r[:, columns] for i, r in enumerate(refs)], axis=0
    )


def dot(a, b, dims=((1,), (0,))):
    return lax.dot_general(a, b, (dims, ((), ())), preferred_element_type=F32)


def select_body(width, experts, *refs):
    tokens, outs, onehot = refs[:5], refs[5:9], refs[9]
    rows = jnp.concatenate([r[...] for r in tokens], axis=0)
    meta = rows[:, rows.shape[1] - META :]
    count = rows.shape[0]
    i = lax.broadcasted_iota(jnp.int32, (TOP, META), 0)
    j = lax.broadcasted_iota(jnp.int32, (TOP, META), 1)
    ids = dot((i == j).astype(BF), meta, ((1,), (1,)))
    chosen = [
        jnp.sum((ids == experts[k].astype(F32)).astype(F32), axis=0, keepdims=True)
        for k in range(4)
    ]
    i = lax.broadcasted_iota(jnp.int32, (count, count), 0)
    j = lax.broadcasted_iota(jnp.int32, (count, count), 1)
    earlier = ((i // TOK_MB == j // TOK_MB) & (i < j)).astype(F32).astype(BF)
    stacked = jnp.concatenate(chosen + chosen, axis=0)
    before = dot(stacked.astype(BF), earlier)
    target = jnp.where(stacked > 0.5, before, -1.0)
    slots = count // TOK_MB * CAP
    r = lax.broadcasted_iota(jnp.int32, (slots, count), 0)
    c = lax.broadcasted_iota(jnp.int32, (slots, count), 1)
    wanted = jnp.where(r // CAP == c // TOK_MB, r % CAP, -2).astype(F32)
    for k in range(4):
        onehot[k * slots : (k + 1) * slots] = (target[k : k + 1] == wanted).astype(F32).astype(BF)
    out_pieces(dot(onehot[...], rows[:, :width]).astype(BF), outs)


def select(tokens, experts, width):
    count = sum(t.shape[0] for t in tokens)
    slots = 4 * (count // TOK_MB * CAP)
    outs = pl.pallas_call(
        lambda *refs: select_body(width, *refs),
        out_shape=[jax.ShapeDtypeStruct((n, width), BF) for n in piece_rows(slots)]
        + [jax.ShapeDtypeStruct((slots, count), BF)],
        grid_spec=pltpu.PrefetchScalarGridSpec(
            num_scalar_prefetch=1, grid=(), in_specs=[vmem()] * 5, out_specs=[vmem()] * 5
        ),
        compiler_params=params(12),
        interpret=INTERPRET,
        name="select",
    )(experts, *tokens)
    return outs[:4], outs[4]


def spread_body(*refs):
    pieces, onehot, outs = refs[:5], refs[5], refs[6:]
    total = dot(onehot[...], in_rows(pieces, slice(None)), ((0,), (0,))).astype(BF)
    start = 0
    for out in outs:
        out[...] = total[start : start + out.shape[0]]
        start += out.shape[0]


def spread(pieces, onehot):
    width = pieces[0].shape[1]
    n = onehot.shape[1] // 8
    return pl.pallas_call(
        spread_body,
        out_shape=[jax.ShapeDtypeStruct((k, width), BF) for k in (2 * n, 2 * n, n, n, n, n)],
        in_specs=[vmem()] * 6,
        out_specs=[vmem()] * 6,
        compiler_params=params(12),
        interpret=INTERPRET,
        name="spread",
    )(*pieces, onehot)


def swapped(x):
    size = x.shape[0] // 16
    return jnp.concatenate(
        [x[(a * 4 + b) * size : (a * 4 + b + 1) * size] for b in range(4) for a in range(4)], axis=0
    )


def hidden_body(place, *refs):
    own_a, own_b = refs[:5], refs[5:10]
    peer_a, peer_b = refs[10:12], refs[12:14]
    gate, up, out_a, out_b, x, acc = refs[14:]
    step = pl.program_id(0)
    block, width = gate.shape
    q = x.shape[0] // 4
    for i, group in enumerate((own_a, own_b)):

        @pl.when(step == i)
        def _(group=group):
            x[...] = in_rows(group, slice(0, block))

    for i, group in enumerate((peer_a, peer_b)):

        @pl.when(step == i + 2)
        def _(group=group):
            x[:q] = group[0][:q, :block]
            x[3 * q :] = group[0][q:, :block]
            x[q : 3 * q] = group[1][:, :block]

    g = dot(x[...], gate[...])
    u = dot(x[...], up[...])
    k = step % 2

    @pl.when(step < 2)
    def _():
        acc[k, :, :width] = g
        acc[k, :, width:] = u

    @pl.when(step >= 2)
    def _():
        acc[k, :, :width] += g
        acc[k, :, width:] += u

    @pl.when(step == 3)
    def _():
        meta = in_rows(own_a, slice(block, block + META))
        i = lax.broadcasted_iota(jnp.int32, (META, META), 0)
        j = lax.broadcasted_iota(jnp.int32, (META, META), 1)
        moved = dot(meta, (i == j + GATES_AT).astype(F32).astype(BF))
        lane = lax.broadcasted_iota(jnp.int32, meta.shape, 1)
        hit = (meta.astype(F32) == place[1].astype(F32)) & (lane < 3 * TOP)
        scale = jnp.sum(jnp.where(hit, moved, 0.0), axis=1, keepdims=True)
        total = acc[0] + swapped(acc[1])
        g, u = total[:, :width], total[:, width:]
        hidden = (g * jax.nn.sigmoid(g) * u * scale).astype(BF)
        out_a[...] = hidden
        out_b[...] = swapped(hidden)


def hidden_of(own_a, own_b, peer_a, peer_b, gate, up, place):
    depth, width = gate.shape
    slots = 4 * own_a[0].shape[0]
    block = depth // 4

    def rows(i, place_ref):
        mine = place_ref[0]
        return jnp.where(i < 2, 2 * mine + i, 2 * (1 - mine) + i - 2), 0

    weight = pl.BlockSpec((block, width), rows)
    return pl.pallas_call(
        hidden_body,
        out_shape=[jax.ShapeDtypeStruct((slots, width), BF)] * 2,
        grid_spec=pltpu.PrefetchScalarGridSpec(
            num_scalar_prefetch=1,
            grid=(4,),
            in_specs=[vmem()] * 14 + [weight, weight],
            out_specs=[vmem()] * 2,
            scratch_shapes=[
                pltpu.VMEM((slots, block), BF),
                pltpu.VMEM((2, slots, 2 * width), F32),
            ],
        ),
        compiler_params=params(28),
        interpret=INTERPRET,
        name="hidden",
    )(place, *own_a, *own_b, *peer_a, *peer_b, gate, up)


def down_body(t, hidden, weight, out):
    out[...] = dot(hidden[...], weight[...]).astype(BF)


def down_add_body(t, hidden, weight, term, *outs):
    total = dot(hidden[...], weight[...]) + term[...].astype(F32)
    out_pieces(total.astype(BF), outs)


def down(hidden, weight, which, first, term=None):
    slots, inner = hidden.shape
    block = weight.shape[1] // 8
    columns = pl.BlockSpec((inner, block), lambda i, t: (0, 2 * (first + i) + t[0]))
    ins = [pl.BlockSpec((slots, inner), lambda i, t: (0, 0)), columns]
    if term is None:
        sizes, body, args = [slots], down_body, ()
    else:
        sizes, body, args = piece_rows(slots), down_add_body, (term,)
        ins.append(pl.BlockSpec((slots, block), lambda i, t: (0, i)))
    outs = pl.pallas_call(
        body,
        out_shape=[jax.ShapeDtypeStruct((n, 2 * block), BF) for n in sizes],
        grid_spec=pltpu.PrefetchScalarGridSpec(
            num_scalar_prefetch=1,
            grid=(2,),
            in_specs=ins,
            out_specs=[pl.BlockSpec((n, block), lambda i, t: (0, i)) for n in sizes],
        ),
        compiler_params=params(12),
        interpret=INTERPRET,
        name="down" if term is None else "down_add",
    )(which, hidden, weight, *args)
    return outs[0] if term is None else outs


def peer_rows(pieces):
    here, got, far_a, far_b, left = pieces
    near = jnp.concatenate([here, left], axis=0)
    rest = jnp.concatenate([got[: here.shape[0]], far_a, far_b], axis=0)
    return [shift(near, "tp", 1), shift(rest, "tp", 1)]


def local(tokens, gates, expert_ids, gate_weight, up_weight, down_weight):
    gate, up, downw = gate_weight[0], up_weight[0], down_weight[0]
    y, x, zl, t = (lax.axis_index(a).astype(jnp.int32) for a in ("y", "x", "zl", "tp"))
    half = tokens.shape[1] // 2
    ids = expert_ids.astype(BF)
    high = lax.reduce_precision(gates, 8, 7)
    middle = lax.reduce_precision(gates - high, 8, 7)
    parts = [high.astype(BF), middle.astype(BF), (gates - high - middle).astype(BF)]
    rows = tokens.shape[0]
    blank = jnp.zeros((rows, GATES_AT - 3 * TOP), BF)
    tail = jnp.zeros((rows, META - GATES_AT - 3 * TOP), BF)
    meta = jnp.concatenate([ids] * 3 + [blank] + parts + [tail], axis=1)
    own_a = jnp.concatenate([tokens[:, :half], meta], axis=1)
    own_b = jnp.concatenate([tokens[:, half:], meta], axis=1)
    offsets = jnp.arange(4, dtype=jnp.int32)
    experts_a = y * 8 + (x + offsets) % 4 * 2 + zl
    experts_b = (y + offsets) % 4 * 8 + x * 2 + zl
    place = jnp.stack([t, y * 8 + x * 2 + zl])
    other_a, other_b = shift(own_a, Z, 1), shift(own_b, Z, -1)
    rows_a, rows_b = ring_gather(own_a, other_a, "y"), ring_gather(own_b, other_b, "x")
    sent_a, onehot_a = select(rows_a, experts_a, half + META)
    got_a = slots_exchange(sent_a, "x")
    sent_b, onehot_b = select(rows_b, experts_b, half)
    got_b = slots_exchange(sent_b, "y")
    peer_a = peer_rows([p[:, :half] for p in got_a])
    peer_b = peer_rows(got_b)
    hid_a, hid_b = hidden_of(got_a, got_b, peer_a, peer_b, gate, up, place)
    which = t.reshape(1)
    term_a = shift(down(hid_a, downw, 1 - which, 0), "tp", 1)
    term_b = shift(down(hid_b, downw, 1 - which, 2), "tp", 1)
    back_a = slots_exchange(down(hid_a, downw, which, 0, term_a), "x")
    back_b = slots_exchange(down(hid_b, downw, which, 2, term_b), "y")
    near_a, away_a = ring_scatter(*spread(back_a, onehot_a), "y")
    near_b, away_b = ring_scatter(*spread(back_b, onehot_b), "x")
    low = zl == 0
    blocks = []
    for near, away in ((near_a, away_a), (near_b, away_b)):
        wide = near.shape[1] // 2
        for columns in (slice(0, wide), slice(wide, 2 * wide)):
            n, a = near[:, columns], away[:, columns]
            blocks += [jnp.where(low, n, a), jnp.where(low, a, n)]
    shares = lax.all_to_all(jnp.stack(blocks), Z, split_axis=0, concat_axis=0, tiled=True)
    return jnp.sum(shares.astype(F32), axis=0).astype(BF)


def solution(mesh):
    fine = Mesh(mesh.devices.reshape(4, 4, 4, 2, 2), ("grp", "y", "x", "zl", "tp"))
    ep = ("y", "x", "zl")
    placed = (
        P(ep, "tp"),
        P(ep, None),
        P(ep, None),
        P(ep, None, ("grp", "tp")),
        P(ep, None, ("grp", "tp")),
        P(ep, ("grp", "tp"), None),
    )
    return jax.shard_map(
        local, mesh=fine, in_specs=placed, out_specs=P(ep, ("grp", "tp")), check_vma=False
    )
```

```python
import jax
import jax.numpy as jnp
from jax import lax
from jax.experimental import pallas as pl
from jax.experimental.pallas import tpu as pltpu
from jax.sharding import PartitionSpec as P

EXPERTS = 32
CAP = 8
MB = 2
INTERPRET = False
BF = jnp.bfloat16
F32 = jnp.float32


def dot(a, b):
    return jnp.dot(a, b, preferred_element_type=F32)


def other_core(a):
    return lax.ppermute(a, "tp", [(0, 1), (1, 0)])


def hidden_body(t, own, peer, gate, up, out, acc):
    step = pl.program_id(0)
    width = gate.shape[1]

    def partial_sums(x):
        g, u = dot(x, gate[...]), dot(x, up[...])

        @pl.when(step == 0)
        def _():
            acc[:, :width] = g
            acc[:, width:] = u

        @pl.when(step > 0)
        def _():
            acc[:, :width] += g
            acc[:, width:] += u

    @pl.when(step < 2)
    def _():
        partial_sums(own[...])

    @pl.when(step >= 2)
    def _():
        partial_sums(peer[...])

    @pl.when(step == 3)
    def _():
        g, u = acc[:, :width], acc[:, width:]
        out[...] = (g * jax.nn.sigmoid(g) * u).astype(BF)


def hidden_of(own, peer, gate, up, t):
    depth, width = gate.shape
    slots = own.shape[0]
    block = depth // 4

    def rows(i, t_ref):
        mine = t_ref[0]
        return jnp.where(i < 2, 2 * mine + i, 2 * (1 - mine) + i - 2), 0

    weight = pl.BlockSpec((block, width), rows)
    return pl.pallas_call(
        hidden_body,
        out_shape=jax.ShapeDtypeStruct((slots, width), BF),
        grid_spec=pltpu.PrefetchScalarGridSpec(
            num_scalar_prefetch=1,
            grid=(4,),
            in_specs=[
                pl.BlockSpec((slots, block), lambda i, t_ref: (0, jnp.minimum(i, 1))),
                pl.BlockSpec((slots, block), lambda i, t_ref: (0, jnp.maximum(i - 2, 0))),
                weight,
                weight,
            ],
            out_specs=pl.BlockSpec((slots, width), lambda i, t_ref: (0, 0)),
            scratch_shapes=[pltpu.VMEM((slots, 2 * width), F32)],
        ),
        interpret=INTERPRET,
        name="hidden",
    )(t, own, peer, gate, up)


def down_body(t, hidden, weight, out):
    out[...] = dot(hidden[...], weight[...]).astype(BF)


def down_add_body(t, hidden, weight, term, out):
    out[...] = (dot(hidden[...], weight[...]) + term[...].astype(F32)).astype(BF)


def down(hidden, weight, which, term=None):
    slots, inner = hidden.shape
    block = weight.shape[1] // 8
    ins = [
        pl.BlockSpec((slots, inner), lambda i, t: (0, 0)),
        pl.BlockSpec((inner, block), lambda i, t: (0, 2 * i + t[0])),
    ]
    piece = pl.BlockSpec((slots, block), lambda i, t: (0, i))
    return pl.pallas_call(
        down_body if term is None else down_add_body,
        out_shape=jax.ShapeDtypeStruct((slots, 4 * block), BF),
        grid_spec=pltpu.PrefetchScalarGridSpec(
            num_scalar_prefetch=1,
            grid=(4,),
            in_specs=ins if term is None else ins + [piece],
            out_specs=piece,
        ),
        interpret=INTERPRET,
        name="down" if term is None else "down_add",
    )(which, hidden, weight, *(() if term is None else (term,)))


def split3(v):
    high = lax.reduce_precision(v, 8, 7)
    middle = lax.reduce_precision(v - high, 8, 7)
    return jnp.concatenate([high, middle, v - high - middle], axis=0).astype(BF)


def local(tokens, gates, expert_ids, gate_weight, up_weight, down_weight):
    gate, up, downw = gate_weight[0], up_weight[0], down_weight[0]
    t = lax.axis_index("tp").astype(jnp.int32).reshape(1)
    count = tokens.shape[0] // MB
    width = tokens.shape[1]
    slots = EXPERTS * CAP
    sent, mixes = [], []
    for m in range(MB):
        part = slice(m * count, (m + 1) * count)
        flat = expert_ids[part].reshape(-1)
        onehot = (flat[:, None] == lax.iota(jnp.int32, EXPERTS)[None, :]).astype(jnp.int32)
        before = jnp.cumsum(onehot, axis=0) - onehot
        slot = jnp.sum(before * onehot, axis=1)
        target = (flat * CAP + slot).reshape(count, -1)
        match = (target[None] == lax.iota(jnp.int32, slots)[:, None, None]).astype(F32)
        placing = jnp.sum(match, axis=2).astype(BF)
        mixes.append(split3(jnp.transpose(jnp.sum(match * gates[part][None], axis=2))))
        sent.append(dot(placing, tokens[part]).astype(BF).reshape(EXPERTS, CAP, width))
    results = []
    for m in range(MB):
        rows = lax.all_to_all(sent[m], "ep", split_axis=0, concat_axis=0, tiled=True)
        rows = rows.reshape(slots, width)
        hidden = hidden_of(rows, other_core(rows), gate, up, t)
        term = other_core(down(hidden, downw, 1 - t))
        out = down(hidden, downw, t, term).reshape(EXPERTS, CAP, width)
        back = lax.all_to_all(out, "ep", split_axis=0, concat_axis=0, tiled=True)
        mixed = dot(mixes[m], back.reshape(slots, width))
        results.append(mixed[:count] + mixed[count : 2 * count] + mixed[2 * count :])
    mixed = jnp.concatenate(results, axis=0).astype(BF)
    blocks = jnp.transpose(mixed.reshape(MB * count, 4, width // 4), (1, 0, 2))
    shares = lax.all_to_all(blocks, "grp", split_axis=0, concat_axis=0, tiled=True)
    return jnp.sum(shares.astype(F32), axis=0).astype(BF)


def solution(mesh):
    placed = (
        P("ep", "tp"),
        P("ep", None),
        P("ep", None),
        P("ep", None, ("grp", "tp")),
        P("ep", None, ("grp", "tp")),
        P("ep", ("grp", "tp"), None),
    )
    return jax.shard_map(
        local, mesh=mesh, in_specs=placed, out_specs=P("ep", ("grp", "tp")), check_vma=False
    )
```

```python
import jax
import jax.numpy as jnp
from jax import lax
from jax.experimental import pallas as pl
from jax.experimental.pallas import tpu as pltpu
from jax.sharding import PartitionSpec as P

EXPERTS = 32
CAP = 8
TOK_MB = 16
INTERPRET = False
BF = jnp.bfloat16
F32 = jnp.float32


def dot(a, b):
    return jnp.dot(a, b, preferred_element_type=F32)


def other_core(a):
    return lax.ppermute(a, "tp", [(0, 1), (1, 0)])


def iota(shape, dim):
    return lax.broadcasted_iota(jnp.int32, shape, dim)


def bits(mask):
    return mask.astype(F32).astype(BF)


def place_body(ids_t, tokens, out, placing):
    @pl.when(pl.program_id(0) == 0)
    def _():
        top, count = ids_t.shape
        rows = placing.shape[0]
        per = rows // EXPERTS
        expert = iota((EXPERTS, count), 0)
        chosen = jnp.zeros((EXPERTS, count), F32)
        for k in range(top):
            chosen += (ids_t[k : k + 1, :] == expert).astype(F32)
        i, j = iota((count, count), 0), iota((count, count), 1)
        before = dot(chosen.astype(BF), bits((i // TOK_MB == j // TOK_MB) & (i < j)))
        target = jnp.where(chosen > 0.5, before, -1.0).astype(BF)
        of_row = bits(iota((rows, EXPERTS), 0) // per == iota((rows, EXPERTS), 1))
        target = dot(of_row, target)
        r, c = iota((rows, count), 0), iota((rows, count), 1)
        hit = (target == (r % CAP).astype(F32)) & (c // TOK_MB == r % per // CAP)
        placing[...] = bits(hit)

    out[...] = dot(placing[...], tokens[...]).astype(BF)


def place(tokens, expert_ids):
    count, width = tokens.shape
    rows = EXPERTS * (count // TOK_MB) * CAP
    block = width // 4
    return pl.pallas_call(
        place_body,
        out_shape=jax.ShapeDtypeStruct((rows, width), BF),
        grid=(4,),
        in_specs=[
            pl.BlockSpec(expert_ids.shape[::-1], lambda i: (0, 0)),
            pl.BlockSpec((count, block), lambda i: (0, i)),
        ],
        out_specs=pl.BlockSpec((rows, block), lambda i: (0, i)),
        scratch_shapes=[pltpu.VMEM((rows, count), BF)],
        interpret=INTERPRET,
        name="place",
    )(jnp.transpose(expert_ids), tokens)


def mixing(gates, expert_ids):
    count = gates.shape[0]
    blocks = count // TOK_MB
    onehot = (expert_ids[:, :, None] == lax.iota(jnp.int32, EXPERTS)).astype(F32)
    chosen = jnp.sum(onehot, axis=1)
    weight = jnp.sum(onehot * gates[:, :, None], axis=1)
    earlier = (iota((TOK_MB, TOK_MB), 1) < iota((TOK_MB, TOK_MB), 0)).astype(F32)
    before = jnp.einsum("ts,bse->bte", earlier, chosen.reshape(blocks, TOK_MB, EXPERTS))
    target = jnp.where(chosen > 0.5, before.reshape(count, EXPERTS), -1.0)[:, :, None]
    column = iota((1, 1, blocks * CAP), 2)
    own = column // CAP == iota((count, 1, 1), 0) // TOK_MB
    hit = own & (target == (column % CAP).astype(F32))
    mix = jnp.where(hit, weight[:, :, None], 0.0).reshape(count, -1)
    high = lax.reduce_precision(mix, 8, 7)
    middle = lax.reduce_precision(mix - high, 8, 7)
    return jnp.concatenate([high, middle, mix - high - middle], axis=0).astype(BF)


def mix_body(mix, rows, out):
    total = dot(mix[...], rows[...])
    n = total.shape[0] // 3
    out[...] = (total[:n] + total[n : 2 * n] + total[2 * n :]).astype(BF)[None]


def mix_rows(mix, rows):
    slots, width = rows.shape
    count = mix.shape[0] // 3
    block = width // 4
    return pl.pallas_call(
        mix_body,
        out_shape=jax.ShapeDtypeStruct((4, count, block), BF),
        grid=(4,),
        in_specs=[
            pl.BlockSpec(mix.shape, lambda i: (0, 0)),
            pl.BlockSpec((slots, block), lambda i: (0, i)),
        ],
        out_specs=pl.BlockSpec((1, count, block), lambda i: (i, 0, 0)),
        interpret=INTERPRET,
        name="mix",
    )(mix, rows)


def down_body(t, hidden, weight, out):
    out[...] = dot(hidden[...], weight[...]).astype(BF)


def down_add_body(t, hidden, weight, low, high, out):
    term = jnp.where(pl.program_id(0) < 2, low[...], high[...])
    out[...] = (dot(hidden[...], weight[...]) + term.astype(F32)).astype(BF)


def down(hidden, weight, which, first):
    slots, inner = hidden.shape
    block = weight.shape[1] // 8
    return pl.pallas_call(
        down_body,
        out_shape=jax.ShapeDtypeStruct((slots, 2 * block), BF),
        grid_spec=pltpu.PrefetchScalarGridSpec(
            num_scalar_prefetch=1,
            grid=(2,),
            in_specs=[
                pl.BlockSpec((slots, inner), lambda i, t: (0, 0)),
                pl.BlockSpec((inner, block), lambda i, t: (0, 2 * (first + i) + t[0])),
            ],
            out_specs=pl.BlockSpec((slots, block), lambda i, t: (0, i)),
        ),
        compiler_params=pltpu.CompilerParams(vmem_limit_bytes=12 << 20),
        interpret=INTERPRET,
        name="down",
    )(which, hidden, weight)


def down_add(hidden, weight, which, low, high):
    slots, inner = hidden.shape
    block = weight.shape[1] // 8
    return pl.pallas_call(
        down_add_body,
        out_shape=jax.ShapeDtypeStruct((slots, 4 * block), BF),
        grid_spec=pltpu.PrefetchScalarGridSpec(
            num_scalar_prefetch=1,
            grid=(4,),
            in_specs=[
                pl.BlockSpec((slots, inner), lambda i, t: (0, 0)),
                pl.BlockSpec((inner, block), lambda i, t: (0, 2 * i + t[0])),
                pl.BlockSpec((slots, block), lambda i, t: (0, jnp.minimum(i, 1))),
                pl.BlockSpec((slots, block), lambda i, t: (0, jnp.maximum(i - 2, 0))),
            ],
            out_specs=pl.BlockSpec((slots, block), lambda i, t: (0, i)),
        ),
        compiler_params=pltpu.CompilerParams(vmem_limit_bytes=16 << 20),
        interpret=INTERPRET,
        name="down_add",
    )(which, hidden, weight, low, high)


def local(tokens, gates, expert_ids, gate_weight, up_weight, down_weight):
    downw = down_weight[0]
    t = lax.axis_index("tp").astype(jnp.int32)
    width = tokens.shape[1]
    gate = gate_weight.reshape(2, width, -1)
    up = up_weight.reshape(2, width, -1)

    def half(weight, which):
        return lax.dynamic_index_in_dim(weight, which, 0, keepdims=False)

    sent = place(tokens, expert_ids)
    mix = mixing(gates, expert_ids)
    slots = sent.shape[0]
    sent = sent.reshape(EXPERTS, -1, width)
    rows = lax.all_to_all(sent, "ep", split_axis=0, concat_axis=0, tiled=True)
    rows = rows.reshape(slots, width)
    peer = other_core(rows)
    g, u = dot(rows, half(gate, t)), dot(rows, half(up, t))
    g, u = g + dot(peer, half(gate, 1 - t)), u + dot(peer, half(up, 1 - t))
    hidden = (g * jax.nn.sigmoid(g) * u).astype(BF)
    which = t.reshape(1)
    low = other_core(down(hidden, downw, 1 - which, 0))
    high = other_core(down(hidden, downw, 1 - which, 2))
    out = down_add(hidden, downw, which, low, high).reshape(EXPERTS, -1, width)
    back = lax.all_to_all(out, "ep", split_axis=0, concat_axis=0, tiled=True)
    blocks = mix_rows(mix, back.reshape(slots, width))
    shares = lax.all_to_all(blocks, "grp", split_axis=0, concat_axis=0, tiled=True)
    return jnp.sum(shares.astype(F32), axis=0).astype(BF)


def solution(mesh):
    placed = (
        P("ep", "tp"),
        P("ep", None),
        P("ep", None),
        P("ep", None, ("grp", "tp")),
        P("ep", None, ("grp", "tp")),
        P("ep", ("grp", "tp"), None),
    )
    return jax.shard_map(
        local, mesh=mesh, in_specs=placed, out_specs=P("ep", ("grp", "tp")), check_vma=False
    )
```

```python
import jax
import jax.numpy as jnp
from jax import lax
from jax.experimental import pallas as pl
from jax.experimental.pallas import tpu as pltpu
from jax.sharding import PartitionSpec as P


EXPERTS = 32
CAP = 8
MB = 2
TOK_MB = 16
INTERPRET = False
BF = jnp.bfloat16
F32 = jnp.float32


def dot(a, b):
    return jnp.dot(a, b, preferred_element_type=F32)


def other_core(a):
    return lax.ppermute(a, "tp", [(0, 1), (1, 0)])


def iota(shape, dim):
    return lax.broadcasted_iota(jnp.int32, shape, dim)


def bits(mask):
    return mask.astype(F32).astype(BF)


def place_body(micro, ids_t, tokens, out, placing):
    @pl.when(pl.program_id(0) == 0)
    def _():
        top, count = ids_t.shape
        rows = placing.shape[0]
        expert = iota((EXPERTS, count), 0)
        chosen = jnp.zeros((EXPERTS, count), F32)
        for k in range(top):
            chosen += (ids_t[k : k + 1, :] == expert).astype(F32)
        i, j = iota((count, count), 0), iota((count, count), 1)
        before = dot(chosen.astype(BF), bits((i // TOK_MB == j // TOK_MB) & (i < j)))
        target = jnp.where(chosen > 0.5, before, -1.0).astype(BF)
        of_row = bits(iota((rows, EXPERTS), 0) // CAP == iota((rows, EXPERTS), 1))
        target = dot(of_row, target)
        r, c = iota((rows, count), 0), iota((rows, count), 1)
        hit = (target == (r % CAP).astype(F32)) & (c // TOK_MB == micro)
        placing[...] = bits(hit)

    out[...] = dot(placing[...], tokens[...]).astype(BF)


def place(tokens, expert_ids, micro):
    count, width = tokens.shape
    rows = EXPERTS * CAP
    block = width // 4
    return pl.pallas_call(
        lambda *refs: place_body(micro, *refs),
        out_shape=jax.ShapeDtypeStruct((rows, width), BF),
        grid=(4,),
        in_specs=[
            pl.BlockSpec(expert_ids.shape[::-1], lambda i: (0, 0)),
            pl.BlockSpec((count, block), lambda i: (0, i)),
        ],
        out_specs=pl.BlockSpec((rows, block), lambda i: (0, i)),
        scratch_shapes=[pltpu.VMEM((rows, count), BF)],
        interpret=INTERPRET,
        name="place",
    )(jnp.transpose(expert_ids), tokens)


def mixing(gates, expert_ids):
    count = gates.shape[0]
    blocks = count // TOK_MB
    onehot = (expert_ids[:, :, None] == lax.iota(jnp.int32, EXPERTS)).astype(F32)
    chosen = jnp.sum(onehot, axis=1)
    weight = jnp.sum(onehot * gates[:, :, None], axis=1)
    earlier = (iota((TOK_MB, TOK_MB), 1) < iota((TOK_MB, TOK_MB), 0)).astype(F32)
    before = jnp.einsum("ts,bse->bte", earlier, chosen.reshape(blocks, TOK_MB, EXPERTS))
    target = jnp.where(chosen > 0.5, before.reshape(count, EXPERTS), -1.0)[:, :, None]
    column = iota((1, 1, blocks * CAP), 2)
    own = column // CAP == iota((count, 1, 1), 0) // TOK_MB
    hit = own & (target == (column % CAP).astype(F32))
    mix = jnp.where(hit, weight[:, :, None], 0.0).reshape(count, -1)
    high = lax.reduce_precision(mix, 8, 7)
    middle = lax.reduce_precision(mix - high, 8, 7)
    return jnp.concatenate([high, middle, mix - high - middle], axis=0).astype(BF)


def mix_body(first, mix, rows, out):
    total = dot(mix[...], rows[...])
    n = total.shape[0] // 3
    out[...] = (total[:n] + total[n : 2 * n] + total[2 * n :]).astype(BF)[None]


def mix_rows(mix, rows, first):
    slots, width = rows.shape
    count = mix.shape[0] // 3
    block = width // 4
    return pl.pallas_call(
        mix_body,
        out_shape=jax.ShapeDtypeStruct((4, count, block), BF),
        grid_spec=pltpu.PrefetchScalarGridSpec(
            num_scalar_prefetch=1,
            grid=(4,),
            in_specs=[
                pl.BlockSpec(mix.shape, lambda i, f: (0, 0)),
                pl.BlockSpec((slots, block), lambda i, f: (0, (i + f[0]) % 4)),
            ],
            out_specs=pl.BlockSpec((1, count, block), lambda i, f: (i, 0, 0)),
        ),
        compiler_params=pltpu.CompilerParams(vmem_limit_bytes=8 << 20),
        interpret=INTERPRET,
        name="mix",
    )(first, mix, rows)


def down_body(t, hidden, weight, out):
    out[...] = dot(hidden[...], weight[...]).astype(BF)


def down_add_body(t, hidden, weight, term, out):
    out[...] = (dot(hidden[...], weight[...]) + term[...].astype(F32)).astype(BF)


def down(hidden, weight, which, term=None):
    slots, inner = hidden.shape
    block = weight.shape[1] // 8
    piece = pl.BlockSpec((slots, block), lambda i, t: (0, i))
    ins = [
        pl.BlockSpec((slots, inner), lambda i, t: (0, 0)),
        pl.BlockSpec((inner, block), lambda i, t: (0, 2 * i + t[0])),
    ]
    return pl.pallas_call(
        down_body if term is None else down_add_body,
        out_shape=jax.ShapeDtypeStruct((slots, 4 * block), BF),
        grid_spec=pltpu.PrefetchScalarGridSpec(
            num_scalar_prefetch=1,
            grid=(4,),
            in_specs=ins if term is None else ins + [piece],
            out_specs=piece,
        ),
        compiler_params=pltpu.CompilerParams(vmem_limit_bytes=12 << 20),
        interpret=INTERPRET,
        name="down" if term is None else "down_add",
    )(which, hidden, weight, *(() if term is None else (term,)))


def layer(tokens, gates, expert_ids, gate_weight, up_weight, down_weight):
    downw = down_weight[0]
    t = lax.axis_index("tp").astype(jnp.int32)
    group = lax.axis_index("grp").astype(jnp.int32).reshape(1)
    which = t.reshape(1)
    count, width = tokens.shape[0] // MB, tokens.shape[1]
    slots = EXPERTS * CAP
    gate = gate_weight.reshape(2, width, -1)
    up = up_weight.reshape(2, width, -1)

    def half(weight, which):
        return lax.dynamic_index_in_dim(weight, which, 0, keepdims=False)

    def exchanged(x):
        x = x.reshape(EXPERTS, CAP, width)
        x = lax.all_to_all(x, "ep", split_axis=0, concat_axis=0, tiled=True)
        return x.reshape(slots, width)

    parts = [slice(m * count, (m + 1) * count) for m in range(MB)]
    results = []
    for m, part in enumerate(parts):
        sent = place(tokens, expert_ids, m)
        mix = mixing(gates[part], expert_ids[part])
        rows = exchanged(sent)
        peer = other_core(rows)
        g, u = dot(rows, half(gate, t)), dot(rows, half(up, t))
        g, u = g + dot(peer, half(gate, 1 - t)), u + dot(peer, half(up, 1 - t))
        hidden = (g * jax.nn.sigmoid(g) * u).astype(BF)
        term = other_core(down(hidden, downw, 1 - which))
        out = down(hidden, downw, which, term)
        back = exchanged(out)
        if m < MB - 1:
            blocks = mix_rows(mix, back, group)
            total = blocks[0].astype(F32)
            for d in (1, 2, 3):
                ring = [(i, (i + d) % 4) for i in range(4)]
                total += lax.ppermute(blocks[d], "grp", ring).astype(F32)
        else:
            blocks = mix_rows(mix, back, jnp.zeros_like(group))
            shares = lax.all_to_all(blocks, "grp", split_axis=0, concat_axis=0, tiled=True)
            total = jnp.sum(shares.astype(F32), axis=0)
        results.append(total.astype(BF))
    return jnp.concatenate(results, axis=0)


def solution(mesh):
    placed = (
        P("ep", "tp"),
        P("ep", None),
        P("ep", None),
        P("ep", None, ("grp", "tp")),
        P("ep", None, ("grp", "tp")),
        P("ep", ("grp", "tp"), None),
    )
    return jax.shard_map(
        layer, mesh=mesh, in_specs=placed, out_specs=P("ep", ("grp", "tp")), check_vma=False
    )
```

```python
import jax
import jax.numpy as jnp
from jax import lax
from jax.experimental import pallas as pl
from jax.experimental.pallas import tpu as pltpu
from jax.sharding import Mesh
from jax.sharding import PartitionSpec as P


EXPERTS = 16
CAP = 8
TOK_MB = 16
INTERPRET = False
BF = jnp.bfloat16
F32 = jnp.float32


def dot(a, b):
    return jnp.dot(a, b, preferred_element_type=F32)


def other_core(a):
    return lax.ppermute(a, "tp", [(0, 1), (1, 0)])


def iota(shape, dim):
    return lax.broadcasted_iota(jnp.int32, shape, dim)


def bits(mask):
    return mask.astype(F32).astype(BF)


def place_body(plane, ids_t, tokens, out, placing):
    @pl.when(pl.program_id(0) == 0)
    def _():
        top, count = ids_t.shape
        rows = placing.shape[0]
        per = rows // EXPERTS
        expert = 2 * iota((EXPERTS, count), 0) + plane[0]
        chosen = jnp.zeros((EXPERTS, count), F32)
        for k in range(top):
            chosen += (ids_t[k : k + 1, :] == expert).astype(F32)
        i, j = iota((count, count), 0), iota((count, count), 1)
        before = dot(chosen.astype(BF), bits((i // TOK_MB == j // TOK_MB) & (i < j)))
        target = jnp.where(chosen > 0.5, before, -1.0).astype(BF)
        of_row = bits(iota((rows, EXPERTS), 0) // per == iota((rows, EXPERTS), 1))
        target = dot(of_row, target)
        r, c = iota((rows, count), 0), iota((rows, count), 1)
        hit = (target == (r % CAP).astype(F32)) & (c // TOK_MB == r % per // CAP)
        placing[...] = bits(hit)

    out[...] = dot(placing[...], tokens[...]).astype(BF)


def place(tokens, ids, plane):
    count, width = tokens.shape
    rows = EXPERTS * (count // TOK_MB) * CAP
    block = width // 4
    return pl.pallas_call(
        place_body,
        out_shape=jax.ShapeDtypeStruct((rows, width), BF),
        grid_spec=pltpu.PrefetchScalarGridSpec(
            num_scalar_prefetch=1,
            grid=(4,),
            in_specs=[
                pl.BlockSpec(ids.shape[::-1], lambda i, p: (0, 0)),
                pl.BlockSpec((count, block), lambda i, p: (0, i)),
            ],
            out_specs=pl.BlockSpec((rows, block), lambda i, p: (0, i)),
            scratch_shapes=[pltpu.VMEM((rows, count), BF)],
        ),
        interpret=INTERPRET,
        name="place",
    )(plane, jnp.transpose(ids), tokens)


def mixing(gates, ids, plane):
    count = gates.shape[0]
    blocks = count // TOK_MB
    onehot = (ids[:, :, None] == 2 * lax.iota(jnp.int32, EXPERTS) + plane).astype(F32)
    chosen = jnp.sum(onehot, axis=1)
    weight = jnp.sum(onehot * gates[:, :, None], axis=1)
    earlier = (iota((TOK_MB, TOK_MB), 1) < iota((TOK_MB, TOK_MB), 0)).astype(F32)
    before = jnp.einsum("ts,bse->bte", earlier, chosen.reshape(blocks, TOK_MB, EXPERTS))
    target = jnp.where(chosen > 0.5, before.reshape(count, EXPERTS), -1.0)[:, :, None]
    column = iota((1, 1, blocks * CAP), 2)
    own = column // CAP == iota((count, 1, 1), 0) // TOK_MB
    hit = own & (target == (column % CAP).astype(F32))
    mix = jnp.where(hit, weight[:, :, None], 0.0).reshape(count, -1)
    high = lax.reduce_precision(mix, 8, 7)
    middle = lax.reduce_precision(mix - high, 8, 7)
    return jnp.concatenate([high, middle, mix - high - middle], axis=0).astype(BF)


def mixed(mix, rows):
    total = dot(mix[...], rows[...])
    n = total.shape[0] // 3
    return (total[:n] + total[n : 2 * n] + total[2 * n :]).astype(BF)


def mix_body(plane, mix, rows, out):
    out[0] = mixed(mix, rows)


def mix_both_body(plane, mix, rows, first, out):
    out[0, plane[0]] = first[0]
    out[0, 1 - plane[0]] = mixed(mix, rows)


def mix_rows(mix, rows, plane, first=None):
    slots, width = rows.shape
    count = mix.shape[0] // 3
    block = width // 4
    one = pl.BlockSpec((1, count, block), lambda i, p: (i, 0, 0))
    ins = [
        pl.BlockSpec(mix.shape, lambda i, p: (0, 0)),
        pl.BlockSpec((slots, block), lambda i, p: (0, i)),
    ]
    if first is None:
        body, shape, spec, args = mix_body, (4, count, block), one, ()
    else:
        body, shape, args = mix_both_body, (4, 2, count, block), (first,)
        spec = pl.BlockSpec((1, 2, count, block), lambda i, p: (i, 0, 0, 0))
        ins.append(one)
    return pl.pallas_call(
        body,
        out_shape=jax.ShapeDtypeStruct(shape, BF),
        grid_spec=pltpu.PrefetchScalarGridSpec(
            num_scalar_prefetch=1, grid=(4,), in_specs=ins, out_specs=spec
        ),
        compiler_params=pltpu.CompilerParams(vmem_limit_bytes=8 << 20),
        interpret=INTERPRET,
        name="mix",
    )(plane, mix, rows, *args)


def down_body(t, hidden, weight, out):
    out[...] = dot(hidden[...], weight[...]).astype(BF)


def down_add_body(t, hidden, weight, term, out):
    out[...] = (dot(hidden[...], weight[...]) + term[...].astype(F32)).astype(BF)


def down(hidden, weight, which, term=None):
    slots, inner = hidden.shape
    block = weight.shape[1] // 8
    piece = pl.BlockSpec((slots, block), lambda i, t: (0, i))
    ins = [
        pl.BlockSpec((slots, inner), lambda i, t: (0, 0)),
        pl.BlockSpec((inner, block), lambda i, t: (0, 2 * i + t[0])),
    ]
    return pl.pallas_call(
        down_body if term is None else down_add_body,
        out_shape=jax.ShapeDtypeStruct((slots, 4 * block), BF),
        grid_spec=pltpu.PrefetchScalarGridSpec(
            num_scalar_prefetch=1,
            grid=(4,),
            in_specs=ins if term is None else ins + [piece],
            out_specs=piece,
        ),
        compiler_params=pltpu.CompilerParams(vmem_limit_bytes=12 << 20),
        interpret=INTERPRET,
        name="down" if term is None else "down_add",
    )(which, hidden, weight, *(() if term is None else (term,)))


def layer(tokens, gates, expert_ids, gate_weight, up_weight, down_weight):
    downw = down_weight[0]
    t = lax.axis_index("tp").astype(jnp.int32)
    plane = lax.axis_index("zl").astype(jnp.int32).reshape(1)
    which = t.reshape(1)
    width = tokens.shape[1]
    gate = gate_weight.reshape(2, width, -1)
    up = up_weight.reshape(2, width, -1)

    def half(weight, which):
        return lax.dynamic_index_in_dim(weight, which, 0, keepdims=False)

    def other_plane(x):
        return lax.ppermute(x, "zl", [(0, 1), (1, 0)])

    def exchanged(x):
        shape = x.shape
        x = x.reshape(EXPERTS, -1, width)
        x = lax.all_to_all(x, ("y", "x"), split_axis=0, concat_axis=0, tiled=True)
        return x.reshape(shape)

    choice = other_plane(jnp.concatenate([expert_ids.astype(F32), gates], axis=1))
    top = expert_ids.shape[1]
    sources = [
        (tokens, expert_ids, gates),
        (other_plane(tokens), choice[:, :top].astype(jnp.int32), choice[:, top:]),
    ]
    blocks = None
    for source, ids, weights in sources:
        sent = place(source, ids, plane)
        mix = mixing(weights, ids, plane)
        rows = exchanged(sent)
        peer = other_core(rows)
        g, u = dot(rows, half(gate, t)), dot(rows, half(up, t))
        g, u = g + dot(peer, half(gate, 1 - t)), u + dot(peer, half(up, 1 - t))
        hidden = (g * jax.nn.sigmoid(g) * u).astype(BF)
        term = other_core(down(hidden, downw, 1 - which))
        out = down(hidden, downw, which, term)
        back = exchanged(out)
        blocks = mix_rows(mix, back, plane, blocks)
    pieces = blocks.reshape(8, *blocks.shape[2:])
    shares = lax.all_to_all(pieces, ("grp", "zl"), split_axis=0, concat_axis=0, tiled=True)
    return jnp.sum(shares.astype(F32), axis=0).astype(BF)


def solution(mesh):
    fine = Mesh(mesh.devices.reshape(4, 4, 4, 2, 2), ("grp", "y", "x", "zl", "tp"))
    ep = ("y", "x", "zl")
    placed = (
        P(ep, "tp"),
        P(ep, None),
        P(ep, None),
        P(ep, None, ("grp", "tp")),
        P(ep, None, ("grp", "tp")),
        P(ep, ("grp", "tp"), None),
    )
    return jax.shard_map(
        layer, mesh=fine, in_specs=placed, out_specs=P(ep, ("grp", "tp")), check_vma=False
    )
```

```python
import jax
import jax.numpy as jnp
from jax import lax
from jax.experimental import pallas as pl
from jax.experimental.pallas import tpu as pltpu
from jax.sharding import PartitionSpec as P


EXPERTS = 32
CAP = 8
MB = 2
TOK_MB = 16
INTERPRET = False
BF = jnp.bfloat16
F32 = jnp.float32


def dot(a, b):
    return jnp.dot(a, b, preferred_element_type=F32)


def other_core(a):
    return lax.ppermute(a, "tp", [(0, 1), (1, 0)])


def iota(shape, dim):
    return lax.broadcasted_iota(jnp.int32, shape, dim)


def bits(mask):
    return mask.astype(F32).astype(BF)


def place_body(micro, ids_t, tokens, out, placing):
    @pl.when(pl.program_id(0) == 0)
    def _():
        top, count = ids_t.shape
        rows = placing.shape[0]
        expert = iota((EXPERTS, count), 0)
        chosen = jnp.zeros((EXPERTS, count), F32)
        for k in range(top):
            chosen += (ids_t[k : k + 1, :] == expert).astype(F32)
        i, j = iota((count, count), 0), iota((count, count), 1)
        before = dot(chosen.astype(BF), bits((i // TOK_MB == j // TOK_MB) & (i < j)))
        target = jnp.where(chosen > 0.5, before, -1.0).astype(BF)
        of_row = bits(iota((rows, EXPERTS), 0) // CAP == iota((rows, EXPERTS), 1))
        target = dot(of_row, target)
        r, c = iota((rows, count), 0), iota((rows, count), 1)
        hit = (target == (r % CAP).astype(F32)) & (c // TOK_MB == micro)
        placing[...] = bits(hit)

    out[...] = dot(placing[...], tokens[...]).astype(BF)


def place(tokens, expert_ids, micro):
    count, width = tokens.shape
    rows = EXPERTS * CAP
    block = width // 2
    return pl.pallas_call(
        lambda *refs: place_body(micro, *refs),
        out_shape=jax.ShapeDtypeStruct((rows, width), BF),
        grid=(2,),
        in_specs=[
            pl.BlockSpec(expert_ids.shape[::-1], lambda i: (0, 0)),
            pl.BlockSpec((count, block), lambda i: (0, i)),
        ],
        out_specs=pl.BlockSpec((rows, block), lambda i: (0, i)),
        scratch_shapes=[pltpu.VMEM((rows, count), BF)],
        interpret=INTERPRET,
        name="place",
    )(jnp.transpose(expert_ids), tokens)


def mixing(gates, expert_ids):
    count = gates.shape[0]
    blocks = count // TOK_MB
    onehot = (expert_ids[:, :, None] == lax.iota(jnp.int32, EXPERTS)).astype(F32)
    chosen = jnp.sum(onehot, axis=1)
    weight = jnp.sum(onehot * gates[:, :, None], axis=1)
    earlier = (iota((TOK_MB, TOK_MB), 1) < iota((TOK_MB, TOK_MB), 0)).astype(F32)
    before = jnp.einsum("ts,bse->bte", earlier, chosen.reshape(blocks, TOK_MB, EXPERTS))
    target = jnp.where(chosen > 0.5, before.reshape(count, EXPERTS), -1.0)[:, :, None]
    column = iota((1, 1, blocks * CAP), 2)
    own = column // CAP == iota((count, 1, 1), 0) // TOK_MB
    hit = own & (target == (column % CAP).astype(F32))
    mix = jnp.where(hit, weight[:, :, None], 0.0).reshape(count, -1)
    high = lax.reduce_precision(mix, 8, 7)
    middle = lax.reduce_precision(mix - high, 8, 7)
    return jnp.concatenate([high, middle, mix - high - middle], axis=0).astype(BF)


def mix_body(first, mix, rows, out):
    total = dot(mix[...], rows[...])
    n = total.shape[0] // 3
    out[...] = (total[:n] + total[n : 2 * n] + total[2 * n :]).astype(BF)[None]


def mix_rows(mix, rows, first):
    slots, width = rows.shape
    count = mix.shape[0] // 3
    block = width // 4
    return pl.pallas_call(
        mix_body,
        out_shape=jax.ShapeDtypeStruct((4, count, block), BF),
        grid_spec=pltpu.PrefetchScalarGridSpec(
            num_scalar_prefetch=1,
            grid=(4,),
            in_specs=[
                pl.BlockSpec(mix.shape, lambda i, f: (0, 0)),
                pl.BlockSpec((slots, block), lambda i, f: (0, (i + f[0]) % 4)),
            ],
            out_specs=pl.BlockSpec((1, count, block), lambda i, f: (i, 0, 0)),
        ),
        compiler_params=pltpu.CompilerParams(vmem_limit_bytes=8 << 20),
        interpret=INTERPRET,
        name="mix",
    )(first, mix, rows)


def mix_last_body(mix, rows, out, acc):
    part = dot(mix[...], rows[...])
    step = pl.program_id(0)

    @pl.when(step == 0)
    def _():
        acc[...] = part

    @pl.when(step == pl.num_programs(0) - 1)
    def _():
        total = acc[...] + part
        blocks, n, block = out.shape
        total = (total[:n] + total[n : 2 * n] + total[2 * n :]).astype(BF)
        for b in range(blocks):
            out[b] = total[:, b * block : (b + 1) * block]


def mix_last(mix, rows):
    slots, width = rows.shape
    count = mix.shape[0] // 3
    half = slots // 2
    return pl.pallas_call(
        mix_last_body,
        out_shape=jax.ShapeDtypeStruct((4, count, width // 4), BF),
        grid=(2,),
        in_specs=[
            pl.BlockSpec((mix.shape[0], half), lambda i: (0, i)),
            pl.BlockSpec((half, width), lambda i: (i, 0)),
        ],
        out_specs=pl.BlockSpec((4, count, width // 4), lambda i: (0, 0, 0)),
        scratch_shapes=[pltpu.VMEM((mix.shape[0], width), F32)],
        compiler_params=pltpu.CompilerParams(vmem_limit_bytes=8 << 20),
        interpret=INTERPRET,
        name="mix_last",
    )(mix, rows)


def down_body(t, hidden, weight, out):
    out[...] = dot(hidden[...], weight[...]).astype(BF)


def down_add_body(t, hidden, weight, term, out):
    out[...] = (dot(hidden[...], weight[...]) + term[...].astype(F32)).astype(BF)


def down(hidden, weight, which, term=None):
    slots, inner = hidden.shape
    block = weight.shape[1] // 8
    piece = pl.BlockSpec((slots, block), lambda i, t: (0, i))
    ins = [
        pl.BlockSpec((slots, inner), lambda i, t: (0, 0)),
        pl.BlockSpec((inner, block), lambda i, t: (0, 2 * i + t[0])),
    ]
    return pl.pallas_call(
        down_body if term is None else down_add_body,
        out_shape=jax.ShapeDtypeStruct((slots, 4 * block), BF),
        grid_spec=pltpu.PrefetchScalarGridSpec(
            num_scalar_prefetch=1,
            grid=(4,),
            in_specs=ins if term is None else ins + [piece],
            out_specs=piece,
        ),
        compiler_params=pltpu.CompilerParams(vmem_limit_bytes=12 << 20),
        interpret=INTERPRET,
        name="down" if term is None else "down_add",
    )(which, hidden, weight, *(() if term is None else (term,)))


def layer(tokens, gates, expert_ids, gate_weight, up_weight, down_weight):
    downw = down_weight[0]
    t = lax.axis_index("tp").astype(jnp.int32)
    group = lax.axis_index("grp").astype(jnp.int32).reshape(1)
    which = t.reshape(1)
    count, width = tokens.shape[0] // MB, tokens.shape[1]
    slots = EXPERTS * CAP
    gate = gate_weight.reshape(2, width, -1)
    up = up_weight.reshape(2, width, -1)

    def half(weight, which):
        return lax.dynamic_index_in_dim(weight, which, 0, keepdims=False)

    def exchanged(x):
        x = x.reshape(EXPERTS, CAP, width)
        x = lax.all_to_all(x, "ep", split_axis=0, concat_axis=0, tiled=True)
        return x.reshape(slots, width)

    parts = [slice(m * count, (m + 1) * count) for m in range(MB)]
    results = []
    for m, part in enumerate(parts):
        sent = place(tokens, expert_ids, m)
        mix = mixing(gates[part], expert_ids[part])
        rows = exchanged(sent)
        peer = other_core(rows)
        g, u = dot(rows, half(gate, t)), dot(rows, half(up, t))
        g, u = g + dot(peer, half(gate, 1 - t)), u + dot(peer, half(up, 1 - t))
        hidden = (g * jax.nn.sigmoid(g) * u).astype(BF)
        term = other_core(down(hidden, downw, 1 - which))
        out = down(hidden, downw, which, term)
        back = exchanged(out)
        if m < MB - 1:
            blocks = mix_rows(mix, back, group)
            total = blocks[0].astype(F32)
            for d in (1, 2, 3):
                ring = [(i, (i + d) % 4) for i in range(4)]
                total += lax.ppermute(blocks[d], "grp", ring).astype(F32)
        else:
            blocks = mix_last(mix, back)
            shares = lax.all_to_all(blocks, "grp", split_axis=0, concat_axis=0, tiled=True)
            total = jnp.sum(shares.astype(F32), axis=0)
        results.append(total.astype(BF))
    return jnp.concatenate(results, axis=0)


def solution(mesh):
    placed = (
        P("ep", "tp"),
        P("ep", None),
        P("ep", None),
        P("ep", None, ("grp", "tp")),
        P("ep", None, ("grp", "tp")),
        P("ep", ("grp", "tp"), None),
    )
    return jax.shard_map(
        layer, mesh=mesh, in_specs=placed, out_specs=P("ep", ("grp", "tp")), check_vma=False
    )
```
